32 devices in a mesh: rows: 8 (over y, x, core), grp: 4 (over z).
Axes of the slice: x: 2, y: 2, z: 4, core: 2. Of those that a mesh axis runs over, the one named last changes fastest.
Arguments:
- momenta: float32 [128, 4, 24576], P('rows', 'grp'), may hold values from -6 to 6
Outputs:
- basis_out: float32 [128, 4, 24576], P(None, 'grp', 'rows')
- factor: float32 [128, 128], replicated
The draws below stay inside these ranges and needn't reach their ends.
All inputs are finite; a program needn't handle non-finite values.
Results may differ from the reference program's by a relative error of at most 0.0003.
Values sent between devices are 32-bit elements; how exact they have to be, the bound alone decides.
No kernel may reach another device: no remote copies, remote signals or barrier semaphores. Data moves between devices by JAX's collectives and lax.ppermute only.
A program may use at most 192 MiB of HBM per device.

```python
import jax
import jax.numpy as jnp

SUBJ = 128
SLABS = 4
SLAB = 24576


def level_of(own_key, shape, pieces, least, largest):
    gain = 1.0
    for axis_at, parts in pieces:
        steps = jax.random.uniform(jax.random.fold_in(jax.random.fold_in(own_key, 6), axis_at), (parts,), jnp.float32, least / len(pieces), largest / len(pieces))
        gain = gain * jnp.repeat(jnp.exp(steps), shape[axis_at] // parts).reshape((-1,) + (1,) * (len(shape) - 1 - axis_at))
    return gain


def bell_draw(stream_key, extent, width, reach, pieces=(), kind=jnp.bfloat16):
    result = width * jax.random.normal(stream_key, extent, jnp.float32)
    if pieces:
        result = result * level_of(stream_key, extent, pieces, -0.22, 0.18)
    return jnp.clip(result, -reach, reach).astype(kind)


def setup_inputs(seed: int = 0) -> dict:
    key_list = jax.random.split(jax.random.key(seed), 2)
    momenta = bell_draw(key_list[0], (SUBJ, SLABS, SLAB), 1.0, 6.0, ((0, 8), (1, 4)), jnp.float32)
    return dict(momenta=momenta)


def reference(momenta):
    all_rows = SLABS * SLAB
    matrix = momenta.reshape(SUBJ, all_rows).T
    ortho, upper_factor = jnp.linalg.qr(matrix)
    signs = jnp.where(jnp.diagonal(upper_factor) < 0, -1.0, 1.0).astype(upper_factor.dtype)
    ortho = ortho * signs[None, :]
    upper_factor = upper_factor * signs[:, None]
    scale = jnp.sqrt(jnp.asarray(all_rows, jnp.float32))
    basis_out = (ortho.T * scale).reshape(SUBJ, SLABS, SLAB).astype(jnp.float32)
    return (basis_out, (upper_factor / scale).astype(jnp.float32))
```

```python
import functools
import math

import jax
import jax.numpy as jnp
from jax import lax
from jax.experimental import pallas as pl
from jax.experimental.pallas import tpu as pltpu
from jax.sharding import PartitionSpec as P

LANES = 128
PANEL = 8


F32 = jnp.float32
BF16 = jnp.bfloat16
VMEM = pl.BlockSpec(memory_space=pltpu.VMEM)
SMEM = pl.BlockSpec(memory_space=pltpu.SMEM)


def swap(x, axis, mask):
    return lax.ppermute(x, axis, [(i, i ^ mask) for i in range(lax.axis_size(axis))])


def gram_kernel(slots, places_ref, *refs):
    pieces, (panel_ref, gram_ref) = refs[:-2], refs[-2:]
    tiles, subjects, _ = panel_ref.shape
    part = subjects // slots
    for slot, piece in enumerate(pieces):
        at = pl.ds(pl.multiple_of(places_ref[slot] * part, part), part)
        for tile in range(tiles):
            panel_ref[tile, at, :] = piece[pl.ds(tile, part, stride=tiles), :]
    total = jnp.zeros(gram_ref.shape, F32)
    for tile in range(tiles):
        rows = panel_ref[tile]
        total += lax.dot_general(
            rows, rows, (((1,), (1,)), ((), ())),
            precision=lax.Precision.HIGHEST, preferred_element_type=F32,
        )
    gram_ref[...] = total


def factor_rows(work_ref, n):
    wide = work_ref.shape[1]
    sub = lax.broadcasted_iota(jnp.int32, (PANEL, 1), 0)
    for start in range(0, n, PANEL):
        rows = work_ref[start:start + PANEL, :]
        columns = [
            jnp.broadcast_to(rows[:, start + j:start + j + 1], (PANEL, LANES))
            for j in range(PANEL)
        ]
        for j in range(PANEL):
            inverse = lax.rsqrt(columns[j][j:j + 1, :])
            below = jnp.where(sub > j, columns[j] * inverse, 0.0)
            done = rows[j:j + 1, :] * jnp.concatenate([inverse] * (wide // LANES), axis=1)
            rows = jnp.where(sub == j, done, rows - jnp.concatenate([below] * (wide // LANES), axis=1) * done)
            for m in range(j + 1, PANEL):
                columns[m] = columns[m] - below * below[m:m + 1, :]
        work_ref[start:start + PANEL, :] = rows
        if start + PANEL < n:
            work_ref[start + PANEL:, :] = work_ref[start + PANEL:, :] - lax.dot_general(
                rows[:, start + PANEL:n], rows, (((0,), (0,)), ((), ())),
                precision=lax.Precision.HIGHEST, preferred_element_type=F32,
            )


def split(x):
    high = x.astype(BF16)
    return high, (x - high.astype(F32)).astype(BF16)


def apply_kernel(scale, gram_ref, panel_ref, basis_ref, factor_ref, work_ref):
    tiles, n, _ = panel_ref.shape
    row = lax.broadcasted_iota(jnp.int32, (n, n), 0)
    col = lax.broadcasted_iota(jnp.int32, (n, n), 1)
    work_ref[:, :n] = gram_ref[...]
    work_ref[:, n:] = jnp.where(row == col, 1.0, 0.0)
    factor_rows(work_ref, n)
    factor_ref[...] = jnp.where(col >= row, work_ref[:, :n] * (1.0 / scale), 0.0)
    high, low = split(work_ref[:, n:] * scale)
    left = jnp.concatenate(
        [jnp.concatenate([high, high], axis=1), jnp.concatenate([low, low], axis=1)], axis=0
    )
    for tile in range(tiles):
        both = jnp.concatenate(split(panel_ref[tile]), axis=0)
        out = jnp.dot(left, both, preferred_element_type=F32)
        basis_ref[pl.ds(tile, n, stride=tiles), :] = out[:n] + out[n:]


def on_device(momenta):
    part, _, length = momenta.shape
    slots = lax.axis_size("rows")
    grps = lax.axis_size("grp")
    n = part * slots
    tiles = length // slots // LANES
    me = lax.axis_index("rows")
    scale = math.sqrt(length * grps)
    blocks = momenta.reshape(part, slots, tiles, LANES)
    pieces = [
        lax.dynamic_index_in_dim(blocks, me ^ mask, 1, keepdims=False).reshape(part * tiles, LANES)
        for mask in range(slots)
    ]
    pieces = [pieces[0]] + [swap(pieces[mask], "rows", mask) for mask in range(1, slots)]
    places = me ^ jnp.arange(slots, dtype=jnp.int32)
    panel, gram = pl.pallas_call(
        functools.partial(gram_kernel, slots),
        out_shape=(
            jax.ShapeDtypeStruct((tiles, n, LANES), F32),
            jax.ShapeDtypeStruct((n, n), F32),
        ),
        in_specs=[SMEM] + [VMEM] * slots,
        out_specs=(VMEM, VMEM),
    )(places, *pieces)
    for axis, size in (("rows", slots), ("grp", grps)):
        mask = 1
        while mask < size:
            gram = gram + swap(gram, axis, mask)
            mask *= 2
    basis, factor = pl.pallas_call(
        functools.partial(apply_kernel, scale),
        out_shape=(
            jax.ShapeDtypeStruct((n * tiles, LANES), F32),
            jax.ShapeDtypeStruct((n, n), F32),
        ),
        in_specs=[VMEM, VMEM],
        out_specs=(VMEM, VMEM),
        scratch_shapes=[pltpu.VMEM((n, 2 * n), F32)],
    )(gram, panel)
    return basis.reshape(n, 1, tiles * LANES), factor


def solution(mesh):
    return jax.shard_map(
        on_device,
        mesh=mesh,
        in_specs=(P("rows", "grp", None),),
        out_specs=(P(None, "grp", "rows"), P()),
        check_vma=False,
    )
```

```python
import functools
import math

import jax
import jax.numpy as jnp
from jax import lax
from jax.experimental import pallas as pl
from jax.experimental.pallas import tpu as pltpu
from jax.sharding import PartitionSpec as P

LANES = 128
SUBLANES = 8
PANEL = 16
PAIR = 2
CHUNK = 8


F32 = jnp.float32
BF16 = jnp.bfloat16
VMEM = pl.BlockSpec(memory_space=pltpu.VMEM)
HBM = pl.BlockSpec(memory_space=pltpu.HBM)
ANY = pl.BlockSpec(memory_space=pl.ANY)
PARAMS = pltpu.CompilerParams(vmem_limit_bytes=16 * 2**20)
NT = (((1,), (1,)), ((), ()))
TN = (((0,), (0,)), ((), ()))


def swap(x, axis, mask):
    return lax.ppermute(x, axis, [(i, i ^ mask) for i in range(lax.axis_size(axis))])


def split(x, parts):
    out = []
    for _ in range(parts):
        out.append(x.astype(BF16))
        x = x - out[-1].astype(F32)
    return out


def spread_lane(x, lane):
    return jnp.take_along_axis(x, jnp.broadcast_to(lane, x.shape), axis=1)


def spread_row(x, row):
    return jnp.broadcast_to(x[row:row + 1, :], x.shape)


def cut_kernel(blocks_ref, *refs):
    pieces, sems = refs[:-1], refs[-1]
    me = lax.axis_index("rows")
    copies = [
        pltpu.make_async_copy(blocks_ref.at[:, me ^ mask], piece, sems.at[mask])
        for mask, piece in enumerate(pieces)
    ]
    for copy in reversed(copies):
        copy.start()
    for copy in reversed(copies):
        copy.wait()


def gram_kernel(order, *refs):
    slots = len(order)
    pieces = refs[:slots]
    pack_ref, panel_ref, panel32_ref, third_ref = refs[slots:]
    tiles, n, _ = third_ref.shape
    part = n // slots
    me = lax.axis_index("rows")
    places = [pl.multiple_of((me ^ slot) * part, part) for slot in order]
    direct = part % 16 == 0
    main = jnp.zeros((2 * n, 2 * n), F32)
    rest = jnp.zeros((n, 2 * n), F32)
    for start in range(0, tiles, PAIR):
        for tile in range(start, start + PAIR):
            for place, piece in zip(places, pieces):
                values = piece[pl.ds(tile, part, stride=tiles), :]
                if direct:
                    high, low, third = split(values, 3)
                    panel_ref[tile, pl.ds(place, part), :] = high
                    panel_ref[tile, pl.ds(n + place, part), :] = low
                    third_ref[tile, pl.ds(place, part), :] = third
                else:
                    panel32_ref[tile, pl.ds(place, part), :] = values
            if not direct:
                high, low, third = split(panel32_ref[tile], 3)
                panel_ref[tile, :n, :] = high
                panel_ref[tile, n:, :] = low
                third_ref[tile] = third
        both = jnp.concatenate([panel_ref[start + i] for i in range(PAIR)], axis=1)
        third = jnp.concatenate([third_ref[start + i] for i in range(PAIR)], axis=1)
        main = main + lax.dot_general(both, both, NT, preferred_element_type=F32)
        rest = rest + lax.dot_general(third, both, NT, preferred_element_type=F32)
    rest = rest[:, :n] + rest[:, n:]
    gram = (main[:n, :n] + main[n:, n:]) + (main[:n, n:] + main[n:, :n]) + (rest + rest.T)
    half, most = n // 2, 3 * n // 4
    lane = lax.broadcasted_iota(jnp.int32, (most - half, n), 1)
    pack_ref[:half] = gram[:half]
    pack_ref[half:] = jnp.where(lane >= half, gram[half:most], pltpu.roll(gram[most:], half, 1))


def factor_rows(work_ref, n):
    subs = PANEL // SUBLANES
    wide = work_ref.shape[1] // LANES
    sub = lax.broadcasted_iota(jnp.int32, (SUBLANES, LANES), 0)

    def at(start, k, w):
        return (
            slice(start + SUBLANES * k, start + SUBLANES * (k + 1)),
            slice(LANES * w, LANES * (w + 1)),
        )

    rows = [[work_ref[at(0, k, w)] for w in range(wide)] for k in range(subs)]
    for start in range(0, n, PANEL):
        after = start + PANEL
        later = None
        if after < n:
            later = [[work_ref[at(after, k, w)] for w in range(wide)] for k in range(subs)]
        columns = [
            [spread_lane(rows[k][0], start + j) if SUBLANES * (k + 1) > j else None for k in range(subs)]
            for j in range(PANEL)
        ]
        for j in range(PANEL):
            home, s = divmod(j, SUBLANES)
            column = columns[j]
            inverse = lax.rsqrt(spread_row(column[home], s))
            square = inverse * inverse
            for m in range(j + 1, PANEL):
                first = m // SUBLANES
                times = spread_row(column[first], m % SUBLANES) * square
                for k in range(first, subs):
                    columns[m][k] = columns[m][k] - column[k] * times
            done = [spread_row(rows[home][w], s) * inverse for w in range(wide)]
            for w in range(wide):
                for k in range(home, subs):
                    lower = column[k] * inverse
                    if k > home:
                        rows[k][w] = rows[k][w] - lower * done[w]
                    else:
                        lower = jnp.where(sub > s, lower, 0.0)
                        rows[k][w] = jnp.where(sub == s, done[w], rows[k][w] - lower * done[w])
            if later is not None:
                for k in range(subs):
                    lower = jnp.take_along_axis(done[0], sub + (after + SUBLANES * k), axis=1)
                    for w in range(wide):
                        later[k][w] = later[k][w] - lower * done[w]
        for k in range(subs):
            for w in range(wide):
                work_ref[at(start, k, w)] = rows[k][w]
        beyond = after + PANEL
        if beyond < n:
            panel = work_ref[start:after, :]
            work_ref[beyond:, :] = work_ref[beyond:, :] - lax.dot_general(
                panel[:, beyond:n], panel, TN,
                precision=lax.Precision.HIGHEST, preferred_element_type=F32,
            )
        rows = later


def apply_kernel(scale, pack_ref, panel_ref, basis_ref, factor_ref, work_ref, upper_ref, out_ref, sems):
    tiles, n, _ = panel_ref.shape
    n = n // 2
    half, most = n // 2, 3 * n // 4
    row = lax.broadcasted_iota(jnp.int32, (n, n), 0)
    col = lax.broadcasted_iota(jnp.int32, (n, n), 1)
    work_ref[:most, :n] = pack_ref[...]
    work_ref[most:, :n] = pltpu.roll(pack_ref[half:], half, 1)
    work_ref[:, n:] = jnp.where(row == col, 1.0, 0.0)
    factor_rows(work_ref, n)
    upper_ref[...] = jnp.where(col >= row, work_ref[:, :n] * (1.0 / scale), 0.0)
    copies = [pltpu.make_async_copy(upper_ref, factor_ref, sems.at[0])]
    copies[0].start()
    high, low = (jnp.concatenate([x, x], axis=1) for x in split(work_ref[:, n:] * scale, 2))
    flat_ref = out_ref.reshape(n * tiles, LANES)
    for tile in range(0, tiles, PAIR):
        both = jnp.concatenate([panel_ref[tile + i] for i in range(PAIR)], axis=1)
        out = jnp.dot(high, both, preferred_element_type=F32)
        out = out + jnp.dot(low, both, preferred_element_type=F32)
        for i in range(PAIR):
            flat_ref[pl.ds(tile + i, n, stride=tiles), :] = out[:, LANES * i:LANES * (i + 1)]
        end = tile + PAIR
        if end % CHUNK == 0:
            part = slice(end - CHUNK, end)
            copies.append(pltpu.make_async_copy(
                out_ref.at[:, part, :], basis_ref.at[:, part, :], sems.at[len(copies)]
            ))
            copies[-1].start()
    for copy in copies:
        copy.wait()


def total_over(x, axis, masks):
    found = {mask: swap(x, axis, mask) for mask in sorted(masks, reverse=True)}
    terms = [x] + [found[mask] for mask in sorted(masks)]
    while len(terms) > 1:
        terms = [a + b for a, b in zip(terms[::2], terms[1::2])]
    return terms[0]


def on_device(momenta):
    part, _, length = momenta.shape
    slots = lax.axis_size("rows")
    grps = lax.axis_size("grp")
    n = part * slots
    tiles = length // slots // LANES
    scale = math.sqrt(length * grps)
    order = sorted(range(slots), key=lambda mask: (-bin(mask >> 1).count("1"), -mask))
    pieces = pl.pallas_call(
        cut_kernel,
        out_shape=[jax.ShapeDtypeStruct((part, tiles, LANES), F32)] * slots,
        in_specs=[HBM],
        out_specs=[VMEM] * slots,
        scratch_shapes=[pltpu.SemaphoreType.DMA((slots,))],
        compiler_params=PARAMS,
    )(pltpu.with_memory_space_constraint(momenta.reshape(part, slots, tiles, LANES), pltpu.HBM))
    pieces = [x.reshape(part * tiles, LANES) for x in pieces]
    for mask in order:
        if mask:
            pieces[mask] = swap(pieces[mask], "rows", mask)
    pack, panel = pl.pallas_call(
        functools.partial(gram_kernel, order),
        out_shape=(
            jax.ShapeDtypeStruct((3 * n // 4, n), F32),
            jax.ShapeDtypeStruct((tiles, 2 * n, LANES), BF16),
        ),
        in_specs=[VMEM] * slots,
        out_specs=(VMEM, VMEM),
        scratch_shapes=[
            pltpu.VMEM((SUBLANES, LANES) if part % 16 == 0 else (tiles, n, LANES), F32),
            pltpu.VMEM((tiles, n, LANES), BF16),
        ],
        compiler_params=PARAMS,
    )(*(pieces[mask] for mask in order))
    mask = 1
    while mask < slots:
        pack = total_over(pack, "rows", [mask])
        mask *= 2
    pack = total_over(pack, "grp", range(1, grps))
    basis, factor = pl.pallas_call(
        functools.partial(apply_kernel, scale),
        out_shape=(
            jax.ShapeDtypeStruct((n, tiles, LANES), F32),
            jax.ShapeDtypeStruct((n, n), F32),
        ),
        in_specs=[VMEM, VMEM],
        out_specs=(ANY, ANY),
        scratch_shapes=[
            pltpu.VMEM((n, 2 * n), F32),
            pltpu.VMEM((n, n), F32),
            pltpu.VMEM((n, tiles, LANES), F32),
            pltpu.SemaphoreType.DMA((1 + tiles // CHUNK,)),
        ],
        compiler_params=PARAMS,
    )(pack, panel)
    return basis.reshape(n, 1, tiles * LANES), factor


def solution(mesh):
    return jax.shard_map(
        on_device,
        mesh=mesh,
        in_specs=(P("rows", "grp", None),),
        out_specs=(P(None, "grp", "rows"), P()),
        check_vma=False,
    )
```

```python
import functools
import math

import jax
import jax.numpy as jnp
from jax import lax
from jax.experimental import pallas as pl
from jax.experimental.pallas import tpu as pltpu
from jax.sharding import PartitionSpec as P

LANES = 128
SUBLANES = 8
PANEL = 16
PAIR = 2
CHUNK = 8


F32 = jnp.float32
BF16 = jnp.bfloat16
VMEM = pl.BlockSpec(memory_space=pltpu.VMEM)
HBM = pl.BlockSpec(memory_space=pltpu.HBM)
ANY = pl.BlockSpec(memory_space=pl.ANY)
PARAMS = pltpu.CompilerParams(vmem_limit_bytes=16 * 2**20)
NT = (((1,), (1,)), ((), ()))
TN = (((0,), (0,)), ((), ()))


def swap(x, axis, mask):
    return lax.ppermute(x, axis, [(i, i ^ mask) for i in range(lax.axis_size(axis))])


def split(x, parts):
    out = []
    for _ in range(parts):
        out.append(x.astype(BF16))
        x = x - out[-1].astype(F32)
    return out


def spread_lane(x, lane):
    return jnp.take_along_axis(x, jnp.broadcast_to(lane, x.shape), axis=1)


def spread_row(x, row):
    return jnp.broadcast_to(x[row:row + 1, :], x.shape)


def cut_kernel(blocks_ref, *refs):
    pieces, sems = refs[:-1], refs[-1]
    me = lax.axis_index("rows")
    copies = [
        pltpu.make_async_copy(blocks_ref.at[:, me ^ mask], piece, sems.at[mask])
        for mask, piece in enumerate(pieces)
    ]
    for copy in reversed(copies):
        copy.start()
    for copy in reversed(copies):
        copy.wait()


def lane_block(index, rows):
    lane = lax.broadcasted_iota(jnp.int32, (rows, LANES), 1)
    return (lane >= PANEL * index) & (lane < PANEL * (index + 1))


def pack_upper(gram, pack_ref):
    n = gram.shape[0]
    blocks = n // PANEL
    half = n // 2
    lane = lax.broadcasted_iota(jnp.int32, (PANEL, n), 1)
    for block in range(blocks // 2):
        at = PANEL * block
        rows = gram[at:at + PANEL]
        if block:
            mirror = gram[n - at - PANEL:n - at]
            rows = jnp.where(lane >= at, rows, pltpu.roll(mirror, at, 1))
        pack_ref[at:at + PANEL] = rows
    last = jnp.zeros((SUBLANES, n), F32)
    for i in range(blocks):
        at = half + SUBLANES * i
        shift = PANEL * i - at // PANEL * PANEL
        rows = pltpu.roll(gram[at:at + SUBLANES], shift % n, 1)
        last = jnp.where(lane_block(i, SUBLANES), rows, last)
    pack_ref[half:] = last


def unpack_upper(pack, work_ref):
    n = pack.shape[1]
    blocks = n // PANEL
    half = n // 2
    for block in range(blocks // 2):
        at = PANEL * block
        rows = pack[at:at + PANEL]
        work_ref[at:at + PANEL, :n] = rows
        mirror = pltpu.roll(rows, (n - at) % n, 1) if block else rows
        for k in range(PANEL // SUBLANES):
            to = n - at - PANEL + SUBLANES * k
            i = (to - half) // SUBLANES
            shift = to // PANEL * PANEL - PANEL * i
            own = pltpu.roll(pack[half:], shift % n, 1)
            work_ref[to:to + SUBLANES, :n] = jnp.where(
                lane_block(to // PANEL, SUBLANES), own, mirror[SUBLANES * k:SUBLANES * (k + 1)]
            )


def gram_kernel(order, *refs):
    slots = len(order)
    pieces = refs[:slots]
    pack_ref, panel_ref, panel32_ref, third_ref = refs[slots:]
    tiles, n, _ = third_ref.shape
    part = n // slots
    me = lax.axis_index("rows")
    places = [pl.multiple_of((me ^ slot) * part, part) for slot in order]
    direct = part % 16 == 0
    main = jnp.zeros((2 * n, 2 * n), F32)
    rest = jnp.zeros((n, 2 * n), F32)
    for start in range(0, tiles, PAIR):
        for tile in range(start, start + PAIR):
            for place, piece in zip(places, pieces):
                values = piece[pl.ds(tile, part, stride=tiles), :]
                if direct:
                    high, low, third = split(values, 3)
                    panel_ref[tile, pl.ds(place, part), :] = high
                    panel_ref[tile, pl.ds(n + place, part), :] = low
                    third_ref[tile, pl.ds(place, part), :] = third
                else:
                    panel32_ref[tile, pl.ds(place, part), :] = values
            if not direct:
                high, low, third = split(panel32_ref[tile], 3)
                panel_ref[tile, :n, :] = high
                panel_ref[tile, n:, :] = low
                third_ref[tile] = third
        both = jnp.concatenate([panel_ref[start + i] for i in range(PAIR)], axis=1)
        third = jnp.concatenate([third_ref[start + i] for i in range(PAIR)], axis=1)
        main = main + lax.dot_general(both, both, NT, preferred_element_type=F32)
        rest = rest + lax.dot_general(third, both, NT, preferred_element_type=F32)
    rest = rest[:, :n] + rest[:, n:]
    gram = (main[:n, :n] + main[n:, n:]) + (main[:n, n:] + main[n:, :n]) + (rest + rest.T)
    pack_upper(gram, pack_ref)


def factor_rows(work_ref, n):
    subs = PANEL // SUBLANES
    wide = work_ref.shape[1] // LANES
    sub = lax.broadcasted_iota(jnp.int32, (SUBLANES, LANES), 0)

    def at(start, k, w):
        return (
            slice(start + SUBLANES * k, start + SUBLANES * (k + 1)),
            slice(LANES * w, LANES * (w + 1)),
        )

    rows = [[work_ref[at(0, k, w)] for w in range(wide)] for k in range(subs)]
    for start in range(0, n, PANEL):
        after = start + PANEL
        later = None
        if after < n:
            later = [[work_ref[at(after, k, w)] for w in range(wide)] for k in range(subs)]
        columns = [
            [spread_lane(rows[k][0], start + j) if SUBLANES * (k + 1) > j else None for k in range(subs)]
            for j in range(PANEL)
        ]
        for j in range(PANEL):
            home, s = divmod(j, SUBLANES)
            column = columns[j]
            inverse = lax.rsqrt(spread_row(column[home], s))
            square = inverse * inverse
            for m in range(j + 1, PANEL):
                first = m // SUBLANES
                times = spread_row(column[first], m % SUBLANES) * square
                for k in range(first, subs):
                    columns[m][k] = columns[m][k] - column[k] * times
            done = [spread_row(rows[home][w], s) * inverse for w in range(wide)]
            for w in range(wide):
                for k in range(home, subs):
                    lower = column[k] * inverse
                    if k > home:
                        rows[k][w] = rows[k][w] - lower * done[w]
                    else:
                        lower = jnp.where(sub > s, lower, 0.0)
                        rows[k][w] = jnp.where(sub == s, done[w], rows[k][w] - lower * done[w])
            if later is not None:
                for k in range(subs):
                    lower = jnp.take_along_axis(done[0], sub + (after + SUBLANES * k), axis=1)
                    for w in range(wide):
                        later[k][w] = later[k][w] - lower * done[w]
        for k in range(subs):
            for w in range(wide):
                work_ref[at(start, k, w)] = rows[k][w]
        beyond = after + PANEL
        if beyond < n:
            panel = work_ref[start:after, :]
            work_ref[beyond:, :] = work_ref[beyond:, :] - lax.dot_general(
                panel[:, beyond:n], panel, TN,
                precision=lax.Precision.HIGHEST, preferred_element_type=F32,
            )
        rows = later


def apply_kernel(scale, pack_ref, panel_ref, basis_ref, factor_ref, work_ref, upper_ref, out_ref, sems):
    tiles, n, _ = panel_ref.shape
    n = n // 2
    row = lax.broadcasted_iota(jnp.int32, (n, n), 0)
    col = lax.broadcasted_iota(jnp.int32, (n, n), 1)
    unpack_upper(pack_ref[...], work_ref)
    work_ref[:, n:] = jnp.where(row == col, 1.0, 0.0)
    factor_rows(work_ref, n)
    upper_ref[...] = jnp.where(col >= row, work_ref[:, :n] * (1.0 / scale), 0.0)
    copies = [pltpu.make_async_copy(upper_ref, factor_ref, sems.at[0])]
    copies[0].start()
    high, low = (jnp.concatenate([x, x], axis=1) for x in split(work_ref[:, n:] * scale, 2))
    flat_ref = out_ref.reshape(n * tiles, LANES)
    for tile in range(0, tiles, PAIR):
        both = jnp.concatenate([panel_ref[tile + i] for i in range(PAIR)], axis=1)
        out = jnp.dot(high, both, preferred_element_type=F32)
        out = out + jnp.dot(low, both, preferred_element_type=F32)
        for i in range(PAIR):
            flat_ref[pl.ds(tile + i, n, stride=tiles), :] = out[:, LANES * i:LANES * (i + 1)]
        end = tile + PAIR
        if end % CHUNK == 0:
            part = slice(end - CHUNK, end)
            copies.append(pltpu.make_async_copy(
                out_ref.at[:, part, :], basis_ref.at[:, part, :], sems.at[len(copies)]
            ))
            copies[-1].start()
    for copy in copies:
        copy.wait()


def cross_swap(x, mask, grp_mask):
    rows, grps = lax.axis_size("rows"), lax.axis_size("grp")
    pairs = [
        (r * grps + g, (r ^ mask) * grps + (g ^ grp_mask)) for r in range(rows) for g in range(grps)
    ]
    return lax.ppermute(x, ("rows", "grp"), pairs)


def add_up(x):
    rows, grps = lax.axis_size("rows"), lax.axis_size("grp")
    x = x + swap(x, "rows", 1)
    mask = 2
    while mask < rows:
        x = x + swap(x, "rows", mask | 1)
        mask *= 2
    found = {mask: cross_swap(x, 1, mask) for mask in range(grps - 1, 0, -1)}
    terms = [x] + [found[mask] for mask in range(1, grps)]
    while len(terms) > 1:
        terms = [a + b for a, b in zip(terms[::2], terms[1::2])]
    return terms[0]


def on_device(momenta):
    part, _, length = momenta.shape
    slots = lax.axis_size("rows")
    grps = lax.axis_size("grp")
    n = part * slots
    tiles = length // slots // LANES
    scale = math.sqrt(length * grps)
    order = sorted(range(slots), key=lambda mask: (-bin(mask >> 1).count("1"), -mask))
    pieces = pl.pallas_call(
        cut_kernel,
        out_shape=[jax.ShapeDtypeStruct((part, tiles, LANES), F32)] * slots,
        in_specs=[HBM],
        out_specs=[VMEM] * slots,
        scratch_shapes=[pltpu.SemaphoreType.DMA((slots,))],
        compiler_params=PARAMS,
    )(pltpu.with_memory_space_constraint(momenta.reshape(part, slots, tiles, LANES), pltpu.HBM))
    pieces = [x.reshape(part * tiles, LANES) for x in pieces]
    for mask in order:
        if mask:
            pieces[mask] = swap(pieces[mask], "rows", mask)
    pack, panel = pl.pallas_call(
        functools.partial(gram_kernel, order),
        out_shape=(
            jax.ShapeDtypeStruct((n // 2 + SUBLANES, n), F32),
            jax.ShapeDtypeStruct((tiles, 2 * n, LANES), BF16),
        ),
        in_specs=[VMEM] * slots,
        out_specs=(VMEM, VMEM),
        scratch_shapes=[
            pltpu.VMEM((SUBLANES, LANES) if part % 16 == 0 else (tiles, n, LANES), F32),
            pltpu.VMEM((tiles, n, LANES), BF16),
        ],
        compiler_params=PARAMS,
    )(*(pieces[mask] for mask in order))
    pack = add_up(pack)
    basis, factor = pl.pallas_call(
        functools.partial(apply_kernel, scale),
        out_shape=(
            jax.ShapeDtypeStruct((n, tiles, LANES), F32),
            jax.ShapeDtypeStruct((n, n), F32),
        ),
        in_specs=[VMEM, VMEM],
        out_specs=(ANY, ANY),
        scratch_shapes=[
            pltpu.VMEM((n, 2 * n), F32),
            pltpu.VMEM((n, n), F32),
            pltpu.VMEM((n, tiles, LANES), F32),
            pltpu.SemaphoreType.DMA((1 + tiles // CHUNK,)),
        ],
        compiler_params=PARAMS,
    )(pack, panel)
    return basis.reshape(n, 1, tiles * LANES), factor


def solution(mesh):
    return jax.shard_map(
        on_device,
        mesh=mesh,
        in_specs=(P("rows", "grp", None),),
        out_specs=(P(None, "grp", "rows"), P()),
        check_vma=False,
    )
```

```python
import functools
import math

import jax
import jax.numpy as jnp
from jax import lax
from jax.experimental import pallas as pl
from jax.experimental.pallas import tpu as pltpu
from jax.sharding import PartitionSpec as P

LANES = 128
SUBLANES = 8
PANEL = 16
PAIR = 2
CHUNK = 8


F32 = jnp.float32
BF16 = jnp.bfloat16
VMEM = pl.BlockSpec(memory_space=pltpu.VMEM)
HBM = pl.BlockSpec(memory_space=pltpu.HBM)
ANY = pl.BlockSpec(memory_space=pl.ANY)
PARAMS = pltpu.CompilerParams(vmem_limit_bytes=16 * 2**20)
NT = (((1,), (1,)), ((), ()))
TN = (((0,), (0,)), ((), ()))


def swap(x, axis, mask):
    return lax.ppermute(x, axis, [(i, i ^ mask) for i in range(lax.axis_size(axis))])


def split(x, parts):
    out = []
    for _ in range(parts):
        out.append(x.astype(BF16))
        x = x - out[-1].astype(F32)
    return out


def spread_lane(x, lane):
    return jnp.take_along_axis(x, jnp.broadcast_to(lane, x.shape), axis=1)


def spread_row(x, row):
    return jnp.broadcast_to(x[row:row + 1, :], x.shape)


def cut_kernel(blocks_ref, *refs):
    pieces, sems = refs[:-1], refs[-1]
    me = lax.axis_index("rows")
    copies = [
        pltpu.make_async_copy(blocks_ref.at[:, me ^ mask], piece, sems.at[mask])
        for mask, piece in enumerate(pieces)
    ]
    for copy in reversed(copies):
        copy.start()
    for copy in reversed(copies):
        copy.wait()


def lane_block(index, rows):
    lane = lax.broadcasted_iota(jnp.int32, (rows, LANES), 1)
    return (lane >= PANEL * index) & (lane < PANEL * (index + 1))


def pack_upper(gram, pack_ref):
    n = gram.shape[0]
    blocks = n // PANEL
    half = n // 2
    lane = lax.broadcasted_iota(jnp.int32, (PANEL, n), 1)
    for block in range(blocks // 2):
        at = PANEL * block
        rows = gram[at:at + PANEL]
        if block:
            mirror = gram[n - at - PANEL:n - at]
            rows = jnp.where(lane >= at, rows, pltpu.roll(mirror, at, 1))
        pack_ref[at:at + PANEL] = rows
    last = jnp.zeros((SUBLANES, n), F32)
    for i in range(blocks):
        at = half + SUBLANES * i
        shift = PANEL * i - at // PANEL * PANEL
        rows = pltpu.roll(gram[at:at + SUBLANES], shift % n, 1)
        last = jnp.where(lane_block(i, SUBLANES), rows, last)
    pack_ref[half:] = last


def unpack_upper(pack, work_ref):
    n = pack.shape[1]
    blocks = n // PANEL
    half = n // 2
    for block in range(blocks // 2):
        at = PANEL * block
        rows = pack[at:at + PANEL]
        work_ref[at:at + PANEL, :n] = rows
        mirror = pltpu.roll(rows, (n - at) % n, 1) if block else rows
        for k in range(PANEL // SUBLANES):
            to = n - at - PANEL + SUBLANES * k
            i = (to - half) // SUBLANES
            shift = to // PANEL * PANEL - PANEL * i
            own = pltpu.roll(pack[half:], shift % n, 1)
            work_ref[to:to + SUBLANES, :n] = jnp.where(
                lane_block(to // PANEL, SUBLANES), own, mirror[SUBLANES * k:SUBLANES * (k + 1)]
            )


def gram_kernel(order, *refs):
    slots = len(order)
    pieces = refs[:slots]
    pack_ref, panel_ref, panel32_ref, third_ref = refs[slots:]
    tiles, n, _ = third_ref.shape
    part = n // slots
    me = lax.axis_index("rows")
    places = [pl.multiple_of((me ^ slot) * part, part) for slot in order]
    direct = part % 16 == 0
    main = jnp.zeros((2 * n, 2 * n), F32)
    rest = jnp.zeros((n, 2 * n), F32)
    for start in range(0, tiles, PAIR):
        for tile in range(start, start + PAIR):
            for place, piece in zip(places, pieces):
                values = piece[pl.ds(tile, part, stride=tiles), :]
                if direct:
                    high, low, third = split(values, 3)
                    panel_ref[tile, pl.ds(place, part), :] = high
                    panel_ref[tile, pl.ds(n + place, part), :] = low
                    third_ref[tile, pl.ds(place, part), :] = third
                else:
                    panel32_ref[tile, pl.ds(place, part), :] = values
            if not direct:
                high, low, third = split(panel32_ref[tile], 3)
                panel_ref[tile, :n, :] = high
                panel_ref[tile, n:, :] = low
                third_ref[tile] = third
        both = jnp.concatenate([panel_ref[start + i] for i in range(PAIR)], axis=1)
        third = jnp.concatenate([third_ref[start + i] for i in range(PAIR)], axis=1)
        main = main + lax.dot_general(both, both, NT, preferred_element_type=F32)
        rest = rest + lax.dot_general(third, both, NT, preferred_element_type=F32)
    rest = rest[:, :n] + rest[:, n:]
    gram = (main[:n, :n] + main[n:, n:]) + (main[:n, n:] + main[n:, :n]) + (rest + rest.T)
    pack_upper(gram, pack_ref)


def factor_rows(work_ref, n):
    subs = PANEL // SUBLANES
    wide = work_ref.shape[1] // LANES
    sub = lax.broadcasted_iota(jnp.int32, (SUBLANES, LANES), 0)

    def at(start, k, w):
        return (
            slice(start + SUBLANES * k, start + SUBLANES * (k + 1)),
            slice(LANES * w, LANES * (w + 1)),
        )

    rows = [[work_ref[at(0, k, w)] for w in range(wide)] for k in range(subs)]
    for start in range(0, n, PANEL):
        after = start + PANEL
        later = None
        if after < n:
            later = [[work_ref[at(after, k, w)] for w in range(wide)] for k in range(subs)]
        columns = [
            [spread_lane(rows[k][0], start + j) if SUBLANES * (k + 1) > j else None for k in range(subs)]
            for j in range(PANEL)
        ]
        for j in range(PANEL):
            home, s = divmod(j, SUBLANES)
            column = columns[j]
            inverse = lax.rsqrt(spread_row(column[home], s))
            square = inverse * inverse
            for m in range(j + 1, PANEL):
                first = m // SUBLANES
                own = spread_row(column[first], m % SUBLANES)
                times = own * square if m > j + 1 else None
                for k in range(first, subs):
                    if m == j + 1:
                        columns[m][k] = columns[m][k] - (column[k] * own) * square
                    else:
                        columns[m][k] = columns[m][k] - column[k] * times
            done = [spread_row(rows[home][w], s) * inverse for w in range(wide)]
            for w in range(wide):
                for k in range(home, subs):
                    lower = column[k] * inverse
                    if k > home:
                        rows[k][w] = rows[k][w] - lower * done[w]
                    else:
                        lower = jnp.where(sub > s, lower, 0.0)
                        rows[k][w] = jnp.where(sub == s, done[w], rows[k][w] - lower * done[w])
            if later is not None:
                for k in range(subs):
                    lower = jnp.take_along_axis(done[0], sub + (after + SUBLANES * k), axis=1)
                    for w in range(wide):
                        later[k][w] = later[k][w] - lower * done[w]
        for k in range(subs):
            for w in range(wide):
                work_ref[at(start, k, w)] = rows[k][w]
        beyond = after + PANEL
        if beyond < n:
            panel = work_ref[start:after, :]
            work_ref[beyond:, :] = work_ref[beyond:, :] - lax.dot_general(
                panel[:, beyond:n], panel, TN,
                precision=lax.Precision.HIGHEST, preferred_element_type=F32,
            )
        rows = later


def apply_kernel(scale, pack_ref, panel_ref, basis_ref, factor_ref, work_ref, upper_ref, out_ref, sems):
    tiles, n, _ = panel_ref.shape
    n = n // 2
    row = lax.broadcasted_iota(jnp.int32, (n, n), 0)
    col = lax.broadcasted_iota(jnp.int32, (n, n), 1)
    unpack_upper(pack_ref[...], work_ref)
    work_ref[:, n:] = jnp.where(row == col, 1.0, 0.0)
    factor_rows(work_ref, n)
    upper_ref[...] = jnp.where(col >= row, work_ref[:, :n] * (1.0 / scale), 0.0)
    copies = [pltpu.make_async_copy(upper_ref, factor_ref, sems.at[0])]
    copies[0].start()
    high, low = (jnp.concatenate([x, x], axis=1) for x in split(work_ref[:, n:] * scale, 2))
    flat_ref = out_ref.reshape(n * tiles, LANES)
    for tile in range(0, tiles, PAIR):
        both = jnp.concatenate([panel_ref[tile + i] for i in range(PAIR)], axis=1)
        out = jnp.dot(high, both, preferred_element_type=F32)
        out = out + jnp.dot(low, both, preferred_element_type=F32)
        for i in range(PAIR):
            flat_ref[pl.ds(tile + i, n, stride=tiles), :] = out[:, LANES * i:LANES * (i + 1)]
        end = tile + PAIR
        if end % CHUNK == 0:
            part = slice(end - CHUNK, end)
            copies.append(pltpu.make_async_copy(
                out_ref.at[:, part, :], basis_ref.at[:, part, :], sems.at[len(copies)]
            ))
            copies[-1].start()
    for copy in copies:
        copy.wait()


def cross_swap(x, mask, grp_mask):
    rows, grps = lax.axis_size("rows"), lax.axis_size("grp")
    pairs = [
        (r * grps + g, (r ^ mask) * grps + (g ^ grp_mask)) for r in range(rows) for g in range(grps)
    ]
    return lax.ppermute(x, ("rows", "grp"), pairs)


def tree(terms):
    while len(terms) > 1:
        terms = [a + b for a, b in zip(terms[::2], terms[1::2])]
    return terms[0]


def add_up(x):
    rows, grps = lax.axis_size("rows"), lax.axis_size("grp")
    x = x + swap(x, "rows", 1)
    mask = 2
    while mask < rows:
        reach = 4 if 2 * mask < rows else 2
        found = {m: swap(x, "rows", m * mask | 1) for m in range(reach - 1, 0, -1)}
        x = tree([x] + [found[m] for m in range(1, reach)])
        mask *= reach
    found = {mask: cross_swap(x, 1, mask) for mask in range(grps - 1, 0, -1)}
    return tree([x] + [found[mask] for mask in range(1, grps)])


def make_apply(n, tiles, scale):
    return pl.pallas_call(
        functools.partial(apply_kernel, scale),
        out_shape=(
            jax.ShapeDtypeStruct((n, tiles, LANES), F32),
            jax.ShapeDtypeStruct((n, n), F32),
        ),
        in_specs=[VMEM, VMEM],
        out_specs=(ANY, ANY),
        scratch_shapes=[
            pltpu.VMEM((n, 2 * n), F32),
            pltpu.VMEM((n, n), F32),
            pltpu.VMEM((n, tiles, LANES), F32),
            pltpu.SemaphoreType.DMA((1 + tiles // CHUNK,)),
        ],
        compiler_params=PARAMS,
    )


def on_device(momenta):
    part, _, length = momenta.shape
    slots = lax.axis_size("rows")
    grps = lax.axis_size("grp")
    n = part * slots
    tiles = length // slots // LANES
    scale = math.sqrt(length * grps)
    order = sorted(range(slots), key=lambda mask: (-bin(mask >> 1).count("1"), -mask))
    pieces = pl.pallas_call(
        cut_kernel,
        out_shape=[jax.ShapeDtypeStruct((part, tiles, LANES), F32)] * slots,
        in_specs=[HBM],
        out_specs=[VMEM] * slots,
        scratch_shapes=[pltpu.SemaphoreType.DMA((slots,))],
        compiler_params=PARAMS,
    )(pltpu.with_memory_space_constraint(momenta.reshape(part, slots, tiles, LANES), pltpu.HBM))
    pieces = [x.reshape(part * tiles, LANES) for x in pieces]
    for mask in order:
        if mask:
            pieces[mask] = swap(pieces[mask], "rows", mask)
    pack, panel = pl.pallas_call(
        functools.partial(gram_kernel, order),
        out_shape=(
            jax.ShapeDtypeStruct((n // 2 + SUBLANES, n), F32),
            jax.ShapeDtypeStruct((tiles, 2 * n, LANES), BF16),
        ),
        in_specs=[VMEM] * slots,
        out_specs=(VMEM, VMEM),
        scratch_shapes=[
            pltpu.VMEM((SUBLANES, LANES) if part % 16 == 0 else (tiles, n, LANES), F32),
            pltpu.VMEM((tiles, n, LANES), BF16),
        ],
        compiler_params=PARAMS,
    )(*(pieces[mask] for mask in order))
    pack = add_up(pack)
    basis, factor = make_apply(n, tiles, scale)(pack, panel)
    return basis.reshape(n, 1, tiles * LANES), factor


def solution(mesh):
    return jax.shard_map(
        on_device,
        mesh=mesh,
        in_specs=(P("rows", "grp", None),),
        out_specs=(P(None, "grp", "rows"), P()),
        check_vma=False,
    )
```

```python
import functools
import math

import jax
import jax.numpy as jnp
from jax import lax
from jax.experimental import pallas as pl
from jax.experimental.pallas import tpu as pltpu
from jax.sharding import PartitionSpec as P

LANES = 128
SUBLANES = 8
PANEL = 16
PAIR = 2
CHUNK = 8
EARLY = 3


F32 = jnp.float32
BF16 = jnp.bfloat16
VMEM = pl.BlockSpec(memory_space=pltpu.VMEM)
HBM = pl.BlockSpec(memory_space=pltpu.HBM)
ANY = pl.BlockSpec(memory_space=pl.ANY)
PARAMS = pltpu.CompilerParams(vmem_limit_bytes=16 * 2**20)
NT = (((1,), (1,)), ((), ()))
TN = (((0,), (0,)), ((), ()))


def swap(x, axis, mask):
    return lax.ppermute(x, axis, [(i, i ^ mask) for i in range(lax.axis_size(axis))])


def split(x, parts):
    out = []
    for _ in range(parts):
        out.append(x.astype(BF16))
        x = x - out[-1].astype(F32)
    return out


def spread_lane(x, lane):
    return jnp.take_along_axis(x, jnp.broadcast_to(lane, x.shape), axis=1)


def spread_row(x, row):
    return jnp.broadcast_to(x[row:row + 1, :], x.shape)


def cut_kernel(blocks_ref, *refs):
    pieces, sems = refs[:-1], refs[-1]
    me = lax.axis_index("rows")
    copies = [
        pltpu.make_async_copy(blocks_ref.at[:, me ^ mask], piece, sems.at[mask])
        for mask, piece in enumerate(pieces)
    ]
    for copy in reversed(copies):
        copy.start()
    for copy in reversed(copies):
        copy.wait()


def lane_block(index, rows):
    lane = lax.broadcasted_iota(jnp.int32, (rows, LANES), 1)
    return (lane >= PANEL * index) & (lane < PANEL * (index + 1))


def pack_upper(gram, pack_ref):
    n = gram.shape[0]
    blocks = n // PANEL
    half = n // 2
    lane = lax.broadcasted_iota(jnp.int32, (PANEL, n), 1)
    for block in range(blocks // 2):
        at = PANEL * block
        rows = gram[at:at + PANEL]
        if block:
            mirror = gram[n - at - PANEL:n - at]
            rows = jnp.where(lane >= at, rows, pltpu.roll(mirror, at, 1))
        pack_ref[at:at + PANEL] = rows
    last = jnp.zeros((SUBLANES, n), F32)
    for i in range(blocks):
        at = half + SUBLANES * i
        shift = PANEL * i - at // PANEL * PANEL
        rows = pltpu.roll(gram[at:at + SUBLANES], shift % n, 1)
        last = jnp.where(lane_block(i, SUBLANES), rows, last)
    pack_ref[half:] = last


def unpack_upper(pack, work_ref):
    n = pack.shape[1]
    blocks = n // PANEL
    half = n // 2
    for block in range(blocks // 2):
        at = PANEL * block
        rows = pack[at:at + PANEL]
        work_ref[at:at + PANEL, :n] = rows
        mirror = pltpu.roll(rows, (n - at) % n, 1) if block else rows
        for k in range(PANEL // SUBLANES):
            to = n - at - PANEL + SUBLANES * k
            i = (to - half) // SUBLANES
            shift = to // PANEL * PANEL - PANEL * i
            own = pltpu.roll(pack[half:], shift % n, 1)
            work_ref[to:to + SUBLANES, :n] = jnp.where(
                lane_block(to // PANEL, SUBLANES), own, mirror[SUBLANES * k:SUBLANES * (k + 1)]
            )


def lay_out(order, slots, tiles, pieces, panel_ref, third_ref):
    count, n, _ = third_ref.shape
    part = n // slots
    me = lax.axis_index("rows")
    places = [pl.multiple_of((me ^ mask) * part, part) for mask in order]
    for tile in tiles:
        for place, piece in zip(places, pieces):
            high, low, third = split(piece[pl.ds(tile, part, stride=count), :], 3)
            panel_ref[tile, pl.ds(place, part), :] = high
            panel_ref[tile, pl.ds(n + place, part), :] = low
            third_ref[tile, pl.ds(place, part), :] = third


def lay_kernel(order, slots, *refs):
    pieces, (panel_ref, third_ref, *staged) = refs[:len(order)], refs[len(order):]
    tiles, n, _ = third_ref.shape
    if not staged:
        lay_out(order, slots, range(tiles), pieces, panel_ref, third_ref)
        return
    part = n // slots
    me = lax.axis_index("rows")
    for tile in range(tiles):
        for mask, piece in zip(order, pieces):
            place = pl.multiple_of((me ^ mask) * part, part)
            staged[0][tile, pl.ds(place, part), :] = piece[pl.ds(tile, part, stride=tiles), :]
    for tile in range(tiles):
        high, low, third = split(staged[0][tile], 3)
        panel_ref[tile, :n, :] = high
        panel_ref[tile, n:, :] = low
        third_ref[tile] = third


def gram_kernel(order, slots, *refs):
    pieces = refs[2:2 + len(order)]
    pack_ref, panel_ref, third_ref = refs[2 + len(order):]
    tiles, n, _ = third_ref.shape
    main = jnp.zeros((2 * n, 2 * n), F32)
    rest = jnp.zeros((n, 2 * n), F32)
    for start in range(0, tiles, PAIR):
        lay_out(order, slots, range(start, start + PAIR), pieces, panel_ref, third_ref)
        both = jnp.concatenate([panel_ref[start + i] for i in range(PAIR)], axis=1)
        third = jnp.concatenate([third_ref[start + i] for i in range(PAIR)], axis=1)
        main = main + lax.dot_general(both, both, NT, preferred_element_type=F32)
        rest = rest + lax.dot_general(third, both, NT, preferred_element_type=F32)
    rest = rest[:, :n] + rest[:, n:]
    gram = (main[:n, :n] + main[n:, n:]) + (main[:n, n:] + main[n:, :n]) + (rest + rest.T)
    pack_upper(gram, pack_ref)


def factor_rows(work_ref, n):
    subs = PANEL // SUBLANES
    wide = work_ref.shape[1] // LANES
    sub = lax.broadcasted_iota(jnp.int32, (SUBLANES, LANES), 0)

    def at(start, k, w):
        return (
            slice(start + SUBLANES * k, start + SUBLANES * (k + 1)),
            slice(LANES * w, LANES * (w + 1)),
        )

    rows = [[work_ref[at(0, k, w)] for w in range(wide)] for k in range(subs)]
    for start in range(0, n, PANEL):
        after = start + PANEL
        later = None
        if after < n:
            later = [[work_ref[at(after, k, w)] for w in range(wide)] for k in range(subs)]
        columns = [
            [spread_lane(rows[k][0], start + j) if SUBLANES * (k + 1) > j else None for k in range(subs)]
            for j in range(PANEL)
        ]
        for j in range(PANEL):
            home, s = divmod(j, SUBLANES)
            column = columns[j]
            inverse = lax.rsqrt(spread_row(column[home], s))
            square = inverse * inverse
            for m in range(j + 1, PANEL):
                first = m // SUBLANES
                own = spread_row(column[first], m % SUBLANES)
                times = own * square if m > j + 1 else None
                for k in range(first, subs):
                    if m == j + 1:
                        columns[m][k] = columns[m][k] - (column[k] * own) * square
                    else:
                        columns[m][k] = columns[m][k] - column[k] * times
            done = [spread_row(rows[home][w], s) * inverse for w in range(wide)]
            for w in range(wide):
                for k in range(home, subs):
                    lower = column[k] * inverse
                    if k > home:
                        rows[k][w] = rows[k][w] - lower * done[w]
                    else:
                        lower = jnp.where(sub > s, lower, 0.0)
                        rows[k][w] = jnp.where(sub == s, done[w], rows[k][w] - lower * done[w])
            if later is not None:
                for k in range(subs):
                    lower = jnp.take_along_axis(done[0], sub + (after + SUBLANES * k), axis=1)
                    for w in range(wide):
                        later[k][w] = later[k][w] - lower * done[w]
        for k in range(subs):
            for w in range(wide):
                work_ref[at(start, k, w)] = rows[k][w]
        beyond = after + PANEL
        if beyond < n:
            panel = work_ref[start:after, :]
            work_ref[beyond:, :] = work_ref[beyond:, :] - lax.dot_general(
                panel[:, beyond:n], panel, TN,
                precision=lax.Precision.HIGHEST, preferred_element_type=F32,
            )
        rows = later


def apply_kernel(scale, pack_ref, panel_ref, basis_ref, factor_ref, work_ref, upper_ref, out_ref, sems):
    tiles, n, _ = panel_ref.shape
    n = n // 2
    row = lax.broadcasted_iota(jnp.int32, (n, n), 0)
    col = lax.broadcasted_iota(jnp.int32, (n, n), 1)
    unpack_upper(pack_ref[...], work_ref)
    work_ref[:, n:] = jnp.where(row == col, 1.0, 0.0)
    factor_rows(work_ref, n)
    upper_ref[...] = jnp.where(col >= row, work_ref[:, :n] * (1.0 / scale), 0.0)
    copies = [pltpu.make_async_copy(upper_ref, factor_ref, sems.at[0])]
    copies[0].start()
    high, low = (jnp.concatenate([x, x], axis=1) for x in split(work_ref[:, n:] * scale, 2))
    flat_ref = out_ref.reshape(n * tiles, LANES)
    for tile in range(0, tiles, PAIR):
        both = jnp.concatenate([panel_ref[tile + i] for i in range(PAIR)], axis=1)
        out = jnp.dot(high, both, preferred_element_type=F32)
        out = out + jnp.dot(low, both, preferred_element_type=F32)
        for i in range(PAIR):
            flat_ref[pl.ds(tile + i, n, stride=tiles), :] = out[:, LANES * i:LANES * (i + 1)]
        end = tile + PAIR
        if end % CHUNK == 0:
            part = slice(end - CHUNK, end)
            copies.append(pltpu.make_async_copy(
                out_ref.at[:, part, :], basis_ref.at[:, part, :], sems.at[len(copies)]
            ))
            copies[-1].start()
    for copy in copies:
        copy.wait()


def cross_swap(x, mask, grp_mask):
    rows, grps = lax.axis_size("rows"), lax.axis_size("grp")
    pairs = [
        (r * grps + g, (r ^ mask) * grps + (g ^ grp_mask)) for r in range(rows) for g in range(grps)
    ]
    return lax.ppermute(x, ("rows", "grp"), pairs)


def tree(terms):
    while len(terms) > 1:
        terms = [a + b for a, b in zip(terms[::2], terms[1::2])]
    return terms[0]


def add_up(x):
    rows, grps = lax.axis_size("rows"), lax.axis_size("grp")
    x = x + swap(x, "rows", 1)
    mask = 2
    while mask < rows:
        reach = 4 if 2 * mask < rows else 2
        found = {m: swap(x, "rows", m * mask | 1) for m in range(reach - 1, 0, -1)}
        x = tree([x] + [found[m] for m in range(1, reach)])
        mask *= reach
    found = {mask: cross_swap(x, 1, mask) for mask in range(grps - 1, 0, -1)}
    return tree([x] + [found[mask] for mask in range(1, grps)])


def make_apply(n, tiles, scale):
    return pl.pallas_call(
        functools.partial(apply_kernel, scale),
        out_shape=(
            jax.ShapeDtypeStruct((n, tiles, LANES), F32),
            jax.ShapeDtypeStruct((n, n), F32),
        ),
        in_specs=[VMEM, VMEM],
        out_specs=(ANY, ANY),
        scratch_shapes=[
            pltpu.VMEM((n, 2 * n), F32),
            pltpu.VMEM((n, n), F32),
            pltpu.VMEM((n, tiles, LANES), F32),
            pltpu.SemaphoreType.DMA((1 + tiles // CHUNK,)),
        ],
        compiler_params=PARAMS,
    )


def on_device(momenta):
    part, _, length = momenta.shape
    slots = lax.axis_size("rows")
    grps = lax.axis_size("grp")
    n = part * slots
    tiles = length // slots // LANES
    scale = math.sqrt(length * grps)
    order = sorted(range(slots), key=lambda mask: (-bin(mask >> 1).count("1"), -mask))
    order[:2] = order[1::-1]
    pieces = pl.pallas_call(
        cut_kernel,
        out_shape=[jax.ShapeDtypeStruct((part, tiles, LANES), F32)] * slots,
        in_specs=[HBM],
        out_specs=[VMEM] * slots,
        scratch_shapes=[pltpu.SemaphoreType.DMA((slots,))],
        compiler_params=PARAMS,
    )(pltpu.with_memory_space_constraint(momenta.reshape(part, slots, tiles, LANES), pltpu.HBM))
    pieces = [x.reshape(part * tiles, LANES) for x in pieces]
    for mask in order:
        if mask:
            pieces[mask] = swap(pieces[mask], "rows", mask)
    whole_tiles = part % (2 * SUBLANES) == 0
    count = EARLY if whole_tiles else slots - 1
    early, late = [0] + order[:count], [mask for mask in order[count:] if mask]
    laid = (
        jax.ShapeDtypeStruct((tiles, 2 * n, LANES), BF16),
        jax.ShapeDtypeStruct((tiles, n, LANES), BF16),
    )
    panel, third = pl.pallas_call(
        functools.partial(lay_kernel, early, slots),
        out_shape=laid,
        in_specs=[VMEM] * len(early),
        out_specs=(VMEM, VMEM),
        scratch_shapes=[] if whole_tiles else [pltpu.VMEM((tiles, n, LANES), F32)],
        compiler_params=PARAMS,
    )(*(pieces[mask] for mask in early))
    pack, panel, _ = pl.pallas_call(
        functools.partial(gram_kernel, late, slots),
        out_shape=(jax.ShapeDtypeStruct((n // 2 + SUBLANES, n), F32), *laid),
        in_specs=[VMEM] * (2 + len(late)),
        out_specs=(VMEM, VMEM, VMEM),
        input_output_aliases={0: 1, 1: 2},
        compiler_params=PARAMS,
    )(panel, third, *(pieces[mask] for mask in late))
    pack = add_up(pack)
    basis, factor = make_apply(n, tiles, scale)(pack, panel)
    return basis.reshape(n, 1, tiles * LANES), factor


def solution(mesh):
    return jax.shard_map(
        on_device,
        mesh=mesh,
        in_specs=(P("rows", "grp", None),),
        out_specs=(P(None, "grp", "rows"), P()),
        check_vma=False,
    )
```
